128 devices in a mesh: row: 16 (over z, y_hi, core), col: 8 (over y_lo, x).
Axes of the slice: x: 4, y: 4 (y_hi: 2, y_lo: 2; y = y_hi * 2 + y_lo), z: 4, core: 2. Of those that a mesh axis runs over, the one named last changes fastest.
Arguments:
- velocity: float32 [3, 128, 128, 128], P(None, 'row', 'col'), may hold values from -6 to 6
Outputs:
- advanced: float32 [3, 128, 128, 128], P(None, 'row', 'col')
The draws below stay inside these ranges and needn't reach their ends.
All inputs are finite; a program needn't handle non-finite values.
Results may differ from the reference program's by a relative error of at most 0.0003.
Values sent between devices are 32-bit elements.
A program may use at most 64 MiB of HBM per device.

```python
import jax
import jax.numpy as jnp

N = 128


def block_levels(key, shape, pieces, least, top_value):
    loudness = 1.0
    for axis_at, shards_of in pieces:
        draws = jax.random.uniform(jax.random.fold_in(jax.random.fold_in(key, 6), axis_at), (shards_of,), jnp.float32, least / len(pieces), top_value / len(pieces))
        loudness = loudness * jnp.repeat(jnp.exp(draws), shape[axis_at] // shards_of).reshape((-1,) + (1,) * (len(shape) - 1 - axis_at))
    return loudness


def scatter_about(key, extent, deviation, bound, shards=(), held_as=jnp.bfloat16):
    loudness = block_levels(key, extent, shards, -0.22, 0.18) if shards else 1.0
    array = jax.random.normal(key, extent, jnp.float32) * deviation * loudness
    return jnp.minimum(jnp.maximum(array, -bound), bound).astype(held_as)


def setup_inputs(seed: int = 0) -> dict:
    arg_keys = jax.random.split(jax.random.key(seed), 2)
    return {
        "velocity": scatter_about(arg_keys[0], (3, N, N, N), 1.0, 6.0, ((1, 16), (2, 8)), jnp.float32),
    }


def spectrum(field):
    return jnp.fft.rfftn(field, axes=(1, 2, 3), norm="forward")[..., : N // 2]


def grid_field(spectral):
    nyquist = jnp.zeros(spectral.shape[:3] + (1,), spectral.dtype)
    padded = jnp.concatenate([spectral, nyquist], axis=3)
    return jnp.fft.irfftn(padded, s=(N, N, N), axes=(1, 2, 3), norm="forward")


def wave_numbers():
    index = jnp.arange(N, dtype=jnp.int32)
    signed = jnp.where(index < N // 2, index, index - N)
    half = jnp.arange(N // 2, dtype=jnp.int32)
    return signed[:, None, None], signed[None, :, None], half[None, None, :]


def cross_with(left, right):
    return jnp.stack([left[1] * right[2] - left[2] * right[1], left[2] * right[0] - left[0] * right[2], left[0] * right[1] - left[1] * right[0]])


def reference(velocity):
    int_waves = wave_numbers()
    mask = ((3 * jnp.abs(int_waves[0]) < N) & (3 * jnp.abs(int_waves[1]) < N) & (3 * jnp.abs(int_waves[2]) < N)).astype(jnp.float32)
    waves = [wave.astype(jnp.float32) for wave in int_waves]
    squared = waves[0] * waves[0] + waves[1] * waves[1] + waves[2] * waves[2]
    safe_norm = jnp.where(squared > 0, squared, jnp.float32(1.0))
    viscous = squared / N
    step = 2.0 / N

    def project(field):
        along = (waves[0] * field[0] + waves[1] * field[1] + waves[2] * field[2]) / safe_norm
        return field - jnp.stack([waves[0] * along, waves[1] * along, waves[2] * along])

    def tendency(state):
        flow = grid_field(state)
        spin = grid_field(1j * cross_with(waves, state))
        product = cross_with(flow, spin)
        return project(mask * spectrum(product)) - viscous * state

    start = project(mask * spectrum(velocity))
    first = tendency(start)
    second = tendency(start + step * first)
    return grid_field(start + 0.5 * step * (first + second)).astype(jnp.float32)
```

```python
import functools

import jax
import jax.numpy as jnp
import numpy as np
from jax import lax
from jax.experimental import pallas as pl
from jax.experimental.pallas import tpu as pltpu
from jax.sharding import PartitionSpec as P

N = 128
BAND = 43
KEPT = 85
PAD = 96
HALF = 64
F32 = jnp.float32
BF16 = jnp.bfloat16
VMEM = pltpu.VMEM
STEP = 2.0 / N


def split_np(table):
    high = table.astype(np.float32).astype(BF16)
    low = (table - high.astype(np.float64)).astype(np.float32).astype(BF16)
    return high, low


def tables():
    turn = 2.0 * np.pi / N
    cell = np.arange(N)
    kz = np.arange(BAND)
    angle_z = turn * ((cell[:, None] * kz[None, :]) % N)
    z_forward = np.zeros((N, N))
    z_forward[:, :BAND] = np.cos(angle_z) / N
    z_forward[:, HALF : HALF + BAND] = -np.sin(angle_z) / N
    weight = np.where(kz == 0, 1.0, 2.0)
    z_inverse = np.zeros((N, N))
    z_inverse[:BAND] = (np.cos(angle_z) * weight).T
    z_inverse[HALF : HALF + BAND] = (-np.sin(angle_z) * weight).T
    z_turned = np.concatenate([z_inverse[HALF:], -z_inverse[:HALF]])
    z_pair = np.concatenate([z_inverse, z_turned])
    wave = np.arange(KEPT)
    wave = np.where(wave < BAND, wave, wave - KEPT)
    angle = turn * ((wave[:, None] * cell[None, :]) % N)
    forward = np.zeros((2 * PAD, N))
    forward[:KEPT] = np.cos(angle) / N
    forward[PAD : PAD + KEPT] = np.sin(angle) / N
    inverse = np.zeros((2 * N, PAD))
    inverse[:N, :KEPT] = np.cos(angle).T
    inverse[N:, :KEPT] = np.sin(angle).T

    def left(table):
        high, low = split_np(table)
        return np.concatenate([high, high, low], axis=1)

    def right(table):
        high, low = split_np(table)
        return np.concatenate([high, high, low], axis=0)

    return right(z_forward), right(z_inverse), right(z_pair), left(forward), left(inverse)


def halves(value):
    high = value.astype(BF16)
    low = (value - high.astype(F32)).astype(BF16)
    return high, low


def times(value, table):
    high, low = halves(value)
    return jnp.dot(
        jnp.concatenate([high, low, high], axis=1), table, preferred_element_type=F32
    )


def under(table, value):
    high, low = halves(value)
    return jnp.dot(
        table, jnp.concatenate([high, low, high], axis=0), preferred_element_type=F32
    )


def column_of(row, col):
    chip = (row // 2) * 8 + col
    spare = jnp.where((chip % 3 == 0) & (chip < 63), 64 + chip // 3, 4096)
    return jnp.where(row % 2 == 1, chip, spare)


def holder_of(column):
    chip = jnp.where(column < 64, column, (column - 64) * 3)
    core = jnp.where(column < 64, 1, 0)
    return (chip // 8) * 2 + core, chip % 8


def kernel(
    v_hbm, zf_hbm, zi_hbm, zp_hbm, xf_hbm, xi_hbm, o_hbm,
    vin, zf, zi, zp, xf, xi, s0, r0, fs, fr, is6, ir6, is3, ir3, t0, q0, out, a0, acc,
    load_sem, store_sem, ready_sem, row_s, row_r, fwd_s, fwd_r, inv_s, inv_r,
):
    row, col = lax.axis_index("row"), lax.axis_index("col")
    me = col * 16 + row
    ki = column_of(row, col)
    active = ki < KEPT
    idle = jnp.logical_not(active)

    loads = [
        pltpu.make_async_copy(src, dst, load_sem.at[n])
        for n, (src, dst) in enumerate(
            [(v_hbm, vin), (zf_hbm, zf), (xf_hbm, xf), (xi_hbm, xi), (zp_hbm, zp), (zi_hbm, zi)]
        )
    ]
    for load in loads:
        load.start()

    barrier = pltpu.get_barrier_semaphore()
    for j in range(1, 16):
        pl.semaphore_signal(barrier, inc=1, device_id=((row + j) % 16, col))
    for j in range(1, 8):
        pl.semaphore_signal(barrier, inc=1, device_id=(row, (col + j) % 8))

    lane = lax.broadcasted_iota(jnp.int32, (1, N), 1)
    side = jnp.where(lane < HALF, 1.0, -1.0).astype(F32)

    def turned(value):
        return pltpu.roll(value, HALF, 1) * side

    def part(value, c):
        return value[:, c * N : (c + 1) * N]

    def fold(both, rows, sign):
        outs = []
        for c in range(both.shape[1] // N):
            piece = part(both, c)
            outs.append(piece[:rows] + sign * turned(piece[rows:]))
        return outs

    def x_forward(parts):
        return fold(under(xf[...], jnp.concatenate(parts, axis=1)), PAD, 1.0)

    def x_inverse_pair(parts):
        return under(xi[...], jnp.concatenate(parts, axis=1))

    def row_exchange(src, dst, slot):
        for j in range(1, 16):
            to = (row + j) % 16
            pltpu.make_async_remote_copy(
                src.at[to], dst.at[row], row_s.at[slot], row_r.at[slot], device_id=(to, col)
            ).start()
        dst[row] = src[row]
        pltpu.make_async_copy(
            dst.at[pl.ds(0, 15)], dst.at[pl.ds(0, 15)], row_r.at[slot]
        ).wait()

    def copy_rows(src, at, dst, to, rows):
        for n in range(rows):
            dst[pl.ds(to * rows + n, 1), :] = src[pl.ds(at * rows + n, 1), :]

    def wait_rows(ref, count, sem):
        pltpu.make_async_copy(ref.at[pl.ds(0, count)], ref.at[pl.ds(0, count)], sem).wait()

    def send_forward(p):
        def body(j, carry):
            i = j + jnp.where(j >= ki, 1, 0)
            pltpu.make_async_remote_copy(
                fs.at[p, pl.ds(i * 3, 3)], fr.at[p, pl.ds(me * 3, 3)],
                fwd_s.at[p], fwd_r.at[p], device_id=holder_of(i),
            ).start()
            return carry

        lax.fori_loop(0, jnp.where(active, KEPT - 1, KEPT), body, 0)

    def put_forward(p, parts):
        for c in range(3):
            fs[p, pl.ds(c, PAD, stride=3), :] = parts[c]

    def take_forward(p):
        copy_rows(fs.at[p], ki, fr.at[p], me, 3)
        wait_rows(fr.at[p], 127 * 3, fwd_r.at[p])
        return [fr[p, pl.ds(c, N, stride=3), :] for c in range(3)]

    def send_inverse(src, dst, p, rows):
        def body(j, carry):
            d = j + jnp.where(j >= me, 1, 0)
            pltpu.make_async_remote_copy(
                src.at[pl.ds(d * rows, rows)], dst.at[pl.ds(ki * rows, rows)],
                inv_s.at[p], inv_r.at[p], device_id=(d % 16, d // 16),
            ).start()
            return carry

        lax.fori_loop(0, 127, body, 0)

    def take_inverse(src, dst, p, rows):
        @pl.when(active)
        def _():
            copy_rows(src, me, dst, ki, rows)
            wait_rows(dst, (KEPT - 1) * rows, inv_r.at[p])

        @pl.when(idle)
        def _():
            wait_rows(dst, KEPT * rows, inv_r.at[p])

        return [dst[pl.ds(c, PAD, stride=rows), :] for c in range(rows)]

    kx = jnp.where(ki < BAND, ki, ki - KEPT).astype(F32)
    ky_at = lax.broadcasted_iota(jnp.int32, (PAD, N), 0)
    ky = jnp.where(ky_at < BAND, ky_at, ky_at - KEPT).astype(F32)
    kz = (lax.broadcasted_iota(jnp.int32, (PAD, N), 1) % HALF).astype(F32)

    def norm():
        return kx * kx + ky * ky + kz * kz

    def spectral(p):
        b = x_forward(take_forward(p))
        squared = norm()
        along = (kx * b[0] + ky * b[1] + kz * b[2]) / jnp.where(squared > 0, squared, 1.0)
        return [b[0] - kx * along, b[1] - ky * along, b[2] - kz * along]

    def scatter(state, ref, rows):
        outs = fold(x_inverse_pair(state), N, -1.0)
        for c in range(rows):
            ref[pl.ds(c, N, stride=rows), :] = outs[c]

    def with_curl(a):
        cross = [
            ky * a[2] - kz * a[1],
            kz * a[0] - kx * a[2],
            kx * a[1] - ky * a[0],
        ]
        return list(a) + [-turned(w) for w in cross]

    loads[0].wait()
    loads[1].wait()
    lines = times(vin[...], zf[...])
    for n in range(24):
        s0[:, n, :] = lines[n * 16 : (n + 1) * 16]
    for p in range(2):
        ir6[p, pl.ds(KEPT * 6, (PAD - KEPT) * 6), :] = jnp.zeros(((PAD - KEPT) * 6, N), F32)
    ir3[pl.ds(KEPT * 3, (PAD - KEPT) * 3), :] = jnp.zeros(((PAD - KEPT) * 3, N), F32)

    pl.semaphore_wait(barrier, 22)
    for j in range(1, 8):
        pl.semaphore_signal(ready_sem, inc=1, device_id=(row, (col + j) % 8))
    row_exchange(s0, r0, 0)
    loads[2].wait()
    put_forward(0, x_forward([r0[:, c * 8 : (c + 1) * 8, :].reshape(N, N) for c in range(3)]))
    pl.semaphore_wait(ready_sem, 7)
    send_forward(0)
    for load in loads[3:]:
        load.wait()

    @pl.when(active)
    def _():
        a = spectral(0)
        for c in range(3):
            a0[c] = a[c]
        scatter(with_curl(a), is6.at[0], 6)
        send_inverse(is6.at[0], ir6.at[0], 0, 6)

    for p in range(2):
        got = take_inverse(is6.at[p], ir6.at[p], p, 6)
        both = x_inverse_pair(got)
        grids = []
        for c in range(6):
            piece = part(both, c)
            grids.append(times(jnp.concatenate([piece[:N], piece[N:]], axis=1), zp[...]))
        u, w = grids[:3], grids[3:]
        product = [
            u[1] * w[2] - u[2] * w[1],
            u[2] * w[0] - u[0] * w[2],
            u[0] * w[1] - u[1] * w[0],
        ]
        put_forward(p + 1, x_forward([times(n, zf[...]) for n in product]))
        send_forward(p + 1)

        @pl.when(active)
        def _():
            b = spectral(p + 1)
            damp = norm() * (1.0 / N)
            if p == 0:
                nxt = []
                for c in range(3):
                    base = a0[c]
                    rate = b[c] - damp * base
                    acc[c] = base + (0.5 * STEP) * rate
                    nxt.append(base + STEP * rate)
                    a0[c] = nxt[c]
                scatter(with_curl(nxt), is6.at[1], 6)
                send_inverse(is6.at[1], ir6.at[1], 1, 6)
            else:
                last = []
                for c in range(3):
                    last.append(acc[c] + (0.5 * STEP) * (b[c] - damp * a0[c]))
                scatter(last, is3, 3)
                send_inverse(is3, ir3, 2, 3)

    got = take_inverse(is3, ir3, 2, 3)
    ends = fold(x_inverse_pair(got), N, -1.0)
    for c in range(3):
        t0[:, c * 8 : (c + 1) * 8, :] = ends[c].reshape(16, 8, N)
    row_exchange(t0, q0, 1)
    final = times(q0[...].reshape(384, N), zi[...])
    for y in range(16):
        for c in range(3):
            at = y * 24 + c * 8
            out[pl.ds(c * 128 + y, 8, stride=16), :] = final[at : at + 8]
    store = pltpu.make_async_copy(out, o_hbm, store_sem)
    store.start()

    for slot in range(2):
        pltpu.make_async_copy(s0.at[pl.ds(0, 15)], s0.at[pl.ds(0, 15)], row_s.at[slot]).wait()
    for p in range(3):
        @pl.when(active)
        def _():
            wait_rows(fs.at[p], (KEPT - 1) * 3, fwd_s.at[p])
            if p < 2:
                wait_rows(is6.at[p], 127 * 6, inv_s.at[p])
            else:
                wait_rows(is3, 127 * 3, inv_s.at[p])

        @pl.when(idle)
        def _():
            wait_rows(fs.at[p], KEPT * 3, fwd_s.at[p])

    store.wait()


def local(velocity):
    consts = tables()
    shapes = [((384, N), F32)] + [(t.shape, BF16) for t in consts]
    scratch = [VMEM(shape, kind) for shape, kind in shapes]
    scratch += [
        VMEM((16, 24, N), F32), VMEM((16, 24, N), F32),
        VMEM((3, PAD * 3, N), F32), VMEM((3, N * 3, N), F32),
        VMEM((2, N * 6, N), F32), VMEM((2, PAD * 6, N), F32),
        VMEM((N * 3, N), F32), VMEM((PAD * 3, N), F32),
        VMEM((16, 24, N), F32), VMEM((16, 24, N), F32),
        VMEM((384, N), F32), VMEM((3, PAD, N), F32), VMEM((3, PAD, N), F32),
        pltpu.SemaphoreType.DMA((6,)), pltpu.SemaphoreType.DMA(()),
        pltpu.SemaphoreType.REGULAR,
        pltpu.SemaphoreType.DMA((2,)), pltpu.SemaphoreType.DMA((2,)),
        pltpu.SemaphoreType.DMA((3,)), pltpu.SemaphoreType.DMA((3,)),
        pltpu.SemaphoreType.DMA((3,)), pltpu.SemaphoreType.DMA((3,)),
    ]
    anywhere = pl.BlockSpec(memory_space=pl.ANY)
    result = pl.pallas_call(
        kernel,
        out_shape=jax.ShapeDtypeStruct((384, N), F32),
        in_specs=[anywhere] * 6,
        out_specs=anywhere,
        scratch_shapes=scratch,
        compiler_params=pltpu.CompilerParams(collective_id=0, has_side_effects=True),
        name="heun",
    )(velocity.reshape(384, N), *[jnp.asarray(t) for t in consts])
    return result.reshape(3, 8, 16, N)


def solution(mesh):
    placed = (P(None, "row", "col", None),)
    return jax.shard_map(
        local, mesh=mesh, in_specs=placed, out_specs=P(None, "row", "col", None), check_vma=False
    )
```

```python
import itertools

import jax
import jax.numpy as jnp
import numpy as np
from jax import lax
from jax.experimental import pallas as pl
from jax.experimental.pallas import tpu as pltpu
from jax.sharding import PartitionSpec as P

N = 128
BAND = 43
KEPT = 85
PAD = 96
HALF = 64
F32 = jnp.float32
BF16 = jnp.bfloat16
VMEM = pltpu.VMEM
STEP = 2.0 / N
MOVES = sorted(
    itertools.product(range(4), repeat=3), key=lambda move: -sum((0, 1, 2, 1)[d] for d in move)
)
ROW_MOVES = [move for move in itertools.product(range(4), range(2), range(2)) if any(move)]
ROW_MOVES.sort(key=lambda move: -((0, 1, 2, 1)[move[0]] + 2 * move[1]))


def split_np(table):
    high = table.astype(np.float32).astype(BF16)
    low = (table - high.astype(np.float64)).astype(np.float32).astype(BF16)
    return high, low


def tables():
    turn = 2.0 * np.pi / N
    cell = np.arange(N)
    kz = np.arange(BAND)
    angle_z = turn * ((cell[:, None] * kz[None, :]) % N)
    z_forward = np.zeros((N, N))
    z_forward[:, :BAND] = np.cos(angle_z) / N
    z_forward[:, HALF : HALF + BAND] = -np.sin(angle_z) / N
    weight = np.where(kz == 0, 1.0, 2.0)
    z_inverse = np.zeros((N, N))
    z_inverse[:BAND] = (np.cos(angle_z) * weight).T
    z_inverse[HALF : HALF + BAND] = (-np.sin(angle_z) * weight).T
    z_turned = np.concatenate([z_inverse[HALF:], -z_inverse[:HALF]])
    z_pair = np.concatenate([z_inverse, z_turned])
    wave = np.arange(KEPT)
    wave = np.where(wave < BAND, wave, wave - KEPT)
    angle = turn * ((wave[:, None] * cell[None, :]) % N)
    forward = np.zeros((2 * PAD, N))
    forward[:KEPT] = np.cos(angle) / N
    forward[PAD : PAD + KEPT] = np.sin(angle) / N
    inverse = np.zeros((2 * N, PAD))
    inverse[:N, :KEPT] = np.cos(angle).T
    inverse[N:, :KEPT] = np.sin(angle).T

    def left(table):
        high, low = split_np(table)
        return np.concatenate([high, high, low], axis=1)

    def right(table):
        high, low = split_np(table)
        return np.concatenate([high, high, low], axis=0)

    return right(z_forward), right(z_inverse), right(z_pair), left(forward), left(inverse)


def halves(value):
    high = value.astype(BF16)
    low = (value - high.astype(F32)).astype(BF16)
    return high, low


def times(value, table):
    high, low = halves(value)
    return jnp.dot(
        jnp.concatenate([high, low, high], axis=1), table, preferred_element_type=F32
    )


def under(table, value):
    high, low = halves(value)
    return jnp.dot(
        table, jnp.concatenate([high, low, high], axis=0), preferred_element_type=F32
    )


def column_of(row, col):
    chip = (row // 2) * 8 + col
    spare = jnp.where((chip % 3 == 0) & (chip < 63), 64 + chip // 3, 4096)
    return jnp.where(row % 2 == 1, chip, spare)


def kernel(
    v_hbm, zf_hbm, zi_hbm, zp_hbm, xf_hbm, xi_hbm, o_hbm,
    vin, zf, zi, zp, xf, xi, s0, r0, fs, fr, is6, ir6, is3, ir3, t0, q0, out, a0, acc,
    load_sem, store_sem, ready_sem, row_s, row_r, fwd_s, fwd_r, inv_s, inv_r,
):
    row, col = lax.axis_index("row"), lax.axis_index("col")
    me = col * 16 + row
    ki = column_of(row, col)
    active = ki < KEPT
    idle = jnp.logical_not(active)

    loads = [
        pltpu.make_async_copy(src, dst, load_sem.at[n])
        for n, (src, dst) in enumerate(
            [(v_hbm, vin), (zf_hbm, zf), (xf_hbm, xf), (xi_hbm, xi), (zp_hbm, zp), (zi_hbm, zi)]
        )
    ]
    for load in loads:
        load.start()

    barrier = pltpu.get_barrier_semaphore()
    for j in range(1, 16):
        pl.semaphore_signal(barrier, inc=1, device_id=((row + j) % 16, col))
    for j in range(1, 8):
        pl.semaphore_signal(barrier, inc=1, device_id=(row, (col + j) % 8))

    z_at, y_at, x_at, core = row // 4, (row // 2 % 2) * 2 + col // 4, col % 4, row % 2
    lane = lax.broadcasted_iota(jnp.int32, (1, N), 1)
    side = jnp.where(lane < HALF, 1.0, -1.0).astype(F32)

    def turned(value):
        return pltpu.roll(value, HALF, 1) * side

    def part(value, c):
        return value[:, c * N : (c + 1) * N]

    def fold(both, rows, sign):
        outs = []
        for c in range(both.shape[1] // N):
            piece = part(both, c)
            outs.append(piece[:rows] + sign * turned(piece[rows:]))
        return outs

    def x_forward(parts):
        return fold(under(xf[...], jnp.concatenate(parts, axis=1)), PAD, 1.0)

    def x_inverse_pair(parts):
        return under(xi[...], jnp.concatenate(parts, axis=1))

    def row_exchange(src, dst, slot):
        for move in ROW_MOVES:
            to = (
                (z_at + move[0]) % 4 * 4
                + (row // 2 + move[1]) % 2 * 2
                + (core + move[2]) % 2
            )
            pltpu.make_async_remote_copy(
                src.at[to], dst.at[row], row_s.at[slot], row_r.at[slot], device_id=(to, col)
            ).start()
        dst[row] = src[row]
        pltpu.make_async_copy(
            dst.at[pl.ds(0, 15)], dst.at[pl.ds(0, 15)], row_r.at[slot]
        ).wait()

    def copy_rows(src, at, dst, to, rows):
        for n in range(rows):
            dst[pl.ds(to * rows + n, 1), :] = src[pl.ds(at * rows + n, 1), :]

    def wait_rows(ref, count, sem):
        pltpu.make_async_copy(ref.at[pl.ds(0, count)], ref.at[pl.ds(0, count)], sem).wait()

    def chip_at(move):
        z, y, x = (z_at + move[0]) % 4, (y_at + move[1]) % 4, (x_at + move[2]) % 4
        return z * 4 + (y // 2) * 2, (y % 2) * 4 + x

    def send_forward(p):
        def one(i, to):
            pltpu.make_async_remote_copy(
                fs.at[p, pl.ds(i * 3, 3)], fr.at[p, pl.ds(me * 3, 3)],
                fwd_s.at[p], fwd_r.at[p], device_id=to,
            ).start()

        for move in MOVES:
            base, side_col = chip_at(move)
            chip = (base // 2) * 8 + side_col
            spare = (chip % 3 == 0) & (chip < 63)
            near = move == (0, 0, 0)

            @pl.when(spare & (core == 1) if near else spare)
            def _():
                one(64 + chip // 3, (base, side_col))

            if near:
                @pl.when(core == 0)
                def _():
                    one(chip, (base + 1, side_col))
            else:
                one(chip, (base + 1, side_col))

    def put_forward(p, parts):
        for c in range(3):
            fs[p, pl.ds(c, PAD, stride=3), :] = parts[c]

    def take_forward(p):
        copy_rows(fs.at[p], ki, fr.at[p], me, 3)
        wait_rows(fr.at[p], 127 * 3, fwd_r.at[p])
        return [fr[p, pl.ds(c, N, stride=3), :] for c in range(3)]

    def send_inverse(src, dst, p, rows):
        def one(to):
            d = to[1] * 16 + to[0]
            pltpu.make_async_remote_copy(
                src.at[pl.ds(d * rows, rows)], dst.at[pl.ds(ki * rows, rows)],
                inv_s.at[p], inv_r.at[p], device_id=to,
            ).start()

        for move in MOVES:
            base, side_col = chip_at(move)
            for other in range(2):
                if move != (0, 0, 0) or other:
                    one((base + (core + other) % 2, side_col))

    def take_inverse(src, dst, p, rows):
        @pl.when(active)
        def _():
            copy_rows(src, me, dst, ki, rows)
            wait_rows(dst, (KEPT - 1) * rows, inv_r.at[p])

        @pl.when(idle)
        def _():
            wait_rows(dst, KEPT * rows, inv_r.at[p])

        return [dst[pl.ds(c, PAD, stride=rows), :] for c in range(rows)]

    kx = jnp.where(ki < BAND, ki, ki - KEPT).astype(F32)
    ky_at = lax.broadcasted_iota(jnp.int32, (PAD, N), 0)
    ky = jnp.where(ky_at < BAND, ky_at, ky_at - KEPT).astype(F32)
    kz = (lax.broadcasted_iota(jnp.int32, (PAD, N), 1) % HALF).astype(F32)

    def norm():
        return kx * kx + ky * ky + kz * kz

    def spectral(p):
        b = x_forward(take_forward(p))
        squared = norm()
        along = (kx * b[0] + ky * b[1] + kz * b[2]) / jnp.where(squared > 0, squared, 1.0)
        return [b[0] - kx * along, b[1] - ky * along, b[2] - kz * along]

    def scatter(state, ref, rows):
        outs = fold(x_inverse_pair(state), N, -1.0)
        for c in range(rows):
            ref[pl.ds(c, N, stride=rows), :] = outs[c]

    def with_curl(a):
        cross = [
            ky * a[2] - kz * a[1],
            kz * a[0] - kx * a[2],
            kx * a[1] - ky * a[0],
        ]
        return list(a) + [-turned(w) for w in cross]

    loads[0].wait()
    loads[1].wait()
    lines = times(vin[...], zf[...])
    for n in range(24):
        s0[:, n, :] = lines[n * 16 : (n + 1) * 16]
    for p in range(2):
        ir6[p, pl.ds(KEPT * 6, (PAD - KEPT) * 6), :] = jnp.zeros(((PAD - KEPT) * 6, N), F32)
    ir3[pl.ds(KEPT * 3, (PAD - KEPT) * 3), :] = jnp.zeros(((PAD - KEPT) * 3, N), F32)

    pl.semaphore_wait(barrier, 22)
    for j in range(1, 8):
        pl.semaphore_signal(ready_sem, inc=1, device_id=(row, (col + j) % 8))
    row_exchange(s0, r0, 0)
    loads[2].wait()
    put_forward(0, x_forward([r0[:, c * 8 : (c + 1) * 8, :].reshape(N, N) for c in range(3)]))
    pl.semaphore_wait(ready_sem, 7)
    send_forward(0)
    for load in loads[3:]:
        load.wait()

    @pl.when(active)
    def _():
        a = spectral(0)
        for c in range(3):
            a0[c] = a[c]
        scatter(with_curl(a), is6.at[0], 6)
        send_inverse(is6.at[0], ir6.at[0], 0, 6)

    for p in range(2):
        got = take_inverse(is6.at[p], ir6.at[p], p, 6)
        both = x_inverse_pair(got)
        grids = []
        for c in range(6):
            piece = part(both, c)
            grids.append(times(jnp.concatenate([piece[:N], piece[N:]], axis=1), zp[...]))
        u, w = grids[:3], grids[3:]
        product = [
            u[1] * w[2] - u[2] * w[1],
            u[2] * w[0] - u[0] * w[2],
            u[0] * w[1] - u[1] * w[0],
        ]
        put_forward(p + 1, x_forward([times(n, zf[...]) for n in product]))
        send_forward(p + 1)

        @pl.when(active)
        def _():
            b = spectral(p + 1)
            damp = norm() * (1.0 / N)
            if p == 0:
                nxt = []
                for c in range(3):
                    base = a0[c]
                    rate = b[c] - damp * base
                    acc[c] = base + (0.5 * STEP) * rate
                    nxt.append(base + STEP * rate)
                    a0[c] = nxt[c]
                scatter(with_curl(nxt), is6.at[1], 6)
                send_inverse(is6.at[1], ir6.at[1], 1, 6)
            else:
                last = []
                for c in range(3):
                    last.append(acc[c] + (0.5 * STEP) * (b[c] - damp * a0[c]))
                scatter(last, is3, 3)
                send_inverse(is3, ir3, 2, 3)

    got = take_inverse(is3, ir3, 2, 3)
    ends = fold(x_inverse_pair(got), N, -1.0)
    for c in range(3):
        t0[:, c * 8 : (c + 1) * 8, :] = ends[c].reshape(16, 8, N)
    row_exchange(t0, q0, 1)
    final = times(q0[...].reshape(384, N), zi[...])
    for y in range(16):
        for c in range(3):
            at = y * 24 + c * 8
            out[pl.ds(c * 128 + y, 8, stride=16), :] = final[at : at + 8]
    store = pltpu.make_async_copy(out, o_hbm, store_sem)
    store.start()

    for slot in range(2):
        pltpu.make_async_copy(s0.at[pl.ds(0, 15)], s0.at[pl.ds(0, 15)], row_s.at[slot]).wait()
    for p in range(3):
        @pl.when(active)
        def _():
            wait_rows(fs.at[p], (KEPT - 1) * 3, fwd_s.at[p])
            if p < 2:
                wait_rows(is6.at[p], 127 * 6, inv_s.at[p])
            else:
                wait_rows(is3, 127 * 3, inv_s.at[p])

        @pl.when(idle)
        def _():
            wait_rows(fs.at[p], KEPT * 3, fwd_s.at[p])

    store.wait()


def local(velocity):
    consts = tables()
    shapes = [((384, N), F32)] + [(t.shape, BF16) for t in consts]
    scratch = [VMEM(shape, kind) for shape, kind in shapes]
    scratch += [
        VMEM((16, 24, N), F32), VMEM((16, 24, N), F32),
        VMEM((3, PAD * 3, N), F32), VMEM((3, N * 3, N), F32),
        VMEM((2, N * 6, N), F32), VMEM((2, PAD * 6, N), F32),
        VMEM((N * 3, N), F32), VMEM((PAD * 3, N), F32),
        VMEM((16, 24, N), F32), VMEM((16, 24, N), F32),
        VMEM((384, N), F32), VMEM((3, PAD, N), F32), VMEM((3, PAD, N), F32),
        pltpu.SemaphoreType.DMA((6,)), pltpu.SemaphoreType.DMA(()),
        pltpu.SemaphoreType.REGULAR,
        pltpu.SemaphoreType.DMA((2,)), pltpu.SemaphoreType.DMA((2,)),
        pltpu.SemaphoreType.DMA((3,)), pltpu.SemaphoreType.DMA((3,)),
        pltpu.SemaphoreType.DMA((3,)), pltpu.SemaphoreType.DMA((3,)),
    ]
    anywhere = pl.BlockSpec(memory_space=pl.ANY)
    result = pl.pallas_call(
        kernel,
        out_shape=jax.ShapeDtypeStruct((384, N), F32),
        in_specs=[anywhere] * 6,
        out_specs=anywhere,
        scratch_shapes=scratch,
        compiler_params=pltpu.CompilerParams(collective_id=0, has_side_effects=True),
        name="heun",
    )(velocity.reshape(384, N), *[jnp.asarray(t) for t in consts])
    return result.reshape(3, 8, 16, N)


def solution(mesh):
    placed = (P(None, "row", "col", None),)
    return jax.shard_map(
        local, mesh=mesh, in_specs=placed, out_specs=P(None, "row", "col", None), check_vma=False
    )
```

```python
import itertools

import jax
import jax.numpy as jnp
import numpy as np
from jax import lax
from jax.experimental import pallas as pl
from jax.experimental.pallas import tpu as pltpu
from jax.sharding import PartitionSpec as P

N = 128
BAND = 43
KEPT = 85
PAD = 96
HALF = 64
F32 = jnp.float32
BF16 = jnp.bfloat16
VMEM = pltpu.VMEM
STEP = 2.0 / N
MOVES = sorted(
    itertools.product(range(4), repeat=3), key=lambda move: -sum((0, 1, 2, 1)[d] for d in move)
)
ROW_MOVES = [move for move in itertools.product(range(4), range(2), range(2)) if any(move)]
ROW_MOVES.sort(key=lambda move: -((0, 1, 2, 1)[move[0]] + 2 * move[1]))


def split_np(table):
    high = table.astype(np.float32).astype(BF16)
    low = (table - high.astype(np.float64)).astype(np.float32).astype(BF16)
    return high, low


def tables():
    turn = 2.0 * np.pi / N
    cell = np.arange(N)
    kz = np.arange(BAND)
    angle_z = turn * ((cell[:, None] * kz[None, :]) % N)
    z_forward = np.zeros((N, N))
    z_forward[:, :BAND] = np.cos(angle_z) / N
    z_forward[:, HALF : HALF + BAND] = -np.sin(angle_z) / N
    weight = np.where(kz == 0, 1.0, 2.0)
    z_inverse = np.zeros((N, N))
    z_inverse[:BAND] = (np.cos(angle_z) * weight).T
    z_inverse[HALF : HALF + BAND] = (-np.sin(angle_z) * weight).T
    z_turned = np.concatenate([z_inverse[HALF:], -z_inverse[:HALF]])

    def spares(first, count):
        lanes = np.arange(count) + BAND
        waves = np.arange(count) + first
        return np.concatenate([lanes, lanes + HALF]), np.concatenate([waves, waves + HALF])

    z_third = np.zeros((2, N, N))
    z_third_back = np.zeros((2, N, N))
    for r in range(2):
        lanes, waves = spares(1 + 21 * r, 21)
        z_third[r][:, lanes] = z_forward[:, waves]
        z_third_back[r][lanes] = z_inverse[waves]
    z_third[0][:, HALF] = z_forward[:, 0]
    z_third_back[0][HALF] = z_inverse[0]
    z_fifth = np.zeros((3, N, N))
    for r, count in enumerate((21, 21, 1)):
        lanes, waves = spares(21 * r, count)
        z_fifth[r][lanes] = z_inverse[waves]
    wave = np.arange(KEPT)
    wave = np.where(wave < BAND, wave, wave - KEPT)
    angle = turn * ((wave[:, None] * cell[None, :]) % N)
    forward = np.zeros((2 * PAD, N))
    forward[:KEPT] = np.cos(angle) / N
    forward[PAD : PAD + KEPT] = np.sin(angle) / N
    inverse = np.zeros((2 * N, PAD))
    inverse[:N, :KEPT] = np.cos(angle).T
    inverse[N:, :KEPT] = np.sin(angle).T

    def left(table):
        high, low = split_np(table)
        return np.concatenate([high, high, low], axis=1)

    def right(table):
        high, low = split_np(table)
        return np.concatenate([high, high, low], axis=0)

    def beside(one, other):
        return right(np.concatenate([one, other], axis=1))

    return (
        right(z_forward),
        beside(z_third[0], z_third[1]),
        left(forward),
        left(inverse),
        np.stack([beside(z_inverse, z_fifth[r]) for r in range(3)]),
        np.stack([right(z_turned), right(z_inverse)]),
        np.stack([beside(z_inverse, z_third_back[r]) for r in range(2)]),
    )


def halves(value):
    high = value.astype(BF16)
    low = (value - high.astype(F32)).astype(BF16)
    return high, low


def times(value, table):
    high, low = halves(value)
    return jnp.dot(
        jnp.concatenate([high, low, high], axis=1), table, preferred_element_type=F32
    )


def under(table, value):
    high, low = halves(value)
    return jnp.dot(
        table, jnp.concatenate([high, low, high], axis=0), preferred_element_type=F32
    )


def column_of(row, col):
    chip = (row // 2) * 8 + col
    spare = jnp.where((chip % 3 == 0) & (chip < 63), 64 + chip // 3, 4096)
    return jnp.where(row % 2 == 1, chip, spare)


def kernel(
    v_hbm, zf_hbm, zt_hbm, xf_hbm, xi_hbm, zu_hbm, zw_hbm, zo_hbm, o_hbm,
    vin, zf, zt, xf, xi, zu, zw, zo, s0, r0, fs, fr, is4, ir4, is3, ir3, t0, q0, out, a0, acc,
    load_sem, store_sem, ready_sem, row_s, row_r, fwd_s, fwd_r, inv_s, inv_r,
):
    row, col = lax.axis_index("row"), lax.axis_index("col")
    me = col * 16 + row
    ki = column_of(row, col)
    active = ki < KEPT
    idle = jnp.logical_not(active)

    loads = [
        pltpu.make_async_copy(src, dst, load_sem.at[n])
        for n, (src, dst) in enumerate(
            [
                (v_hbm, vin), (zf_hbm, zf), (zt_hbm, zt), (xf_hbm, xf), (xi_hbm, xi),
                (zu_hbm, zu), (zw_hbm, zw), (zo_hbm, zo),
            ]
        )
    ]
    for load in loads:
        load.start()

    barrier = pltpu.get_barrier_semaphore()
    for j in range(1, 16):
        pl.semaphore_signal(barrier, inc=1, device_id=((row + j) % 16, col))
    for j in range(1, 8):
        pl.semaphore_signal(barrier, inc=1, device_id=(row, (col + j) % 8))

    z_at, y_at, x_at, core = row // 4, (row // 2 % 2) * 2 + col // 4, col % 4, row % 2
    lane = lax.broadcasted_iota(jnp.int32, (1, N), 1)
    side = jnp.where(lane < HALF, 1.0, -1.0).astype(F32)

    def turned(value):
        return pltpu.roll(value, HALF, 1) * side

    def part(value, c):
        return value[:, c * N : (c + 1) * N]

    def fold(both, rows, sign):
        outs = []
        for c in range(both.shape[1] // N):
            piece = part(both, c)
            outs.append(piece[:rows] + sign * turned(piece[rows:]))
        return outs

    def x_forward(parts):
        return fold(under(xf[...], jnp.concatenate(parts, axis=1)), PAD, 1.0)

    def x_inverse_pair(parts):
        return under(xi[...], jnp.concatenate(parts, axis=1))

    def row_exchange(src, dst, slot):
        for move in ROW_MOVES:
            to = (
                (z_at + move[0]) % 4 * 4
                + (row // 2 + move[1]) % 2 * 2
                + (core + move[2]) % 2
            )
            pltpu.make_async_remote_copy(
                src.at[to], dst.at[row], row_s.at[slot], row_r.at[slot], device_id=(to, col)
            ).start()
        dst[row] = src[row]
        pltpu.make_async_copy(
            dst.at[pl.ds(0, 15)], dst.at[pl.ds(0, 15)], row_r.at[slot]
        ).wait()

    def copy_rows(src, at, dst, to, rows):
        for n in range(rows):
            dst[pl.ds(to * rows + n, 1), :] = src[pl.ds(at * rows + n, 1), :]

    def wait_rows(ref, count, sem):
        pltpu.make_async_copy(ref.at[pl.ds(0, count)], ref.at[pl.ds(0, count)], sem).wait()

    def chip_at(move):
        z, y, x = (z_at + move[0]) % 4, (y_at + move[1]) % 4, (x_at + move[2]) % 4
        return z * 4 + (y // 2) * 2, (y % 2) * 4 + x

    def send_forward(p):
        def one(i, to):
            pltpu.make_async_remote_copy(
                fs.at[p, pl.ds(i * 3, 3)], fr.at[p, pl.ds(me * 3, 3)],
                fwd_s.at[p], fwd_r.at[p], device_id=to,
            ).start()

        for move in MOVES:
            base, side_col = chip_at(move)
            chip = (base // 2) * 8 + side_col
            spare = (chip % 3 == 0) & (chip < 63)
            near = move == (0, 0, 0)

            @pl.when(spare & (core == 1) if near else spare)
            def _():
                one(64 + chip // 3, (base, side_col))

            if near:
                @pl.when(core == 0)
                def _():
                    one(chip, (base + 1, side_col))
            else:
                one(chip, (base + 1, side_col))

    def put_forward(p, parts):
        for c in range(3):
            fs[p, pl.ds(c, PAD, stride=3), :] = parts[c]

    def take_forward(p):
        copy_rows(fs.at[p], ki, fr.at[p], me, 3)
        wait_rows(fr.at[p], 127 * 3, fwd_r.at[p])
        return [fr[p, pl.ds(c, N, stride=3), :] for c in range(3)]

    def send_inverse(src, dst, p, rows):
        def one(to):
            d = to[1] * 16 + to[0]
            pltpu.make_async_remote_copy(
                src.at[pl.ds(d * rows, rows)], dst.at[pl.ds(ki * rows, rows)],
                inv_s.at[p], inv_r.at[p], device_id=to,
            ).start()

        for move in MOVES:
            base, side_col = chip_at(move)
            for other in range(2):
                if move != (0, 0, 0) or other:
                    one((base + (core + other) % 2, side_col))

    def take_inverse(src, dst, p, rows):
        @pl.when(active)
        def _():
            copy_rows(src, me, dst, ki, rows)
            wait_rows(dst, (KEPT - 1) * rows, inv_r.at[p])

        @pl.when(idle)
        def _():
            wait_rows(dst, KEPT * rows, inv_r.at[p])

        return [dst[pl.ds(c, PAD, stride=rows), :] for c in range(rows)]

    kx = jnp.where(ki < BAND, ki, ki - KEPT).astype(F32)
    ky_at = lax.broadcasted_iota(jnp.int32, (PAD, N), 0)
    ky = jnp.where(ky_at < BAND, ky_at, ky_at - KEPT).astype(F32)
    kz = (lax.broadcasted_iota(jnp.int32, (PAD, N), 1) % HALF).astype(F32)

    def norm():
        return kx * kx + ky * ky + kz * kz

    def spectral(p):
        b = x_forward(take_forward(p))
        squared = norm()
        along = (kx * b[0] + ky * b[1] + kz * b[2]) / jnp.where(squared > 0, squared, 1.0)
        return [b[0] - kx * along, b[1] - ky * along, b[2] - kz * along]

    def scatter(state, ref, rows):
        outs = fold(x_inverse_pair(state), N, -1.0)
        for c in range(rows):
            ref[pl.ds(c, N, stride=rows), :] = outs[c]

    spare = lane % HALF >= BAND

    def with_curl(a):
        first = -turned(ky * a[2] - kz * a[1])
        last = -turned(kx * a[1] - ky * a[0])
        return [
            jnp.where(spare, pltpu.roll(first, BAND, 1), a[0]),
            jnp.where(spare, pltpu.roll(first, BAND - 21, 1), a[1]),
            jnp.where(spare, pltpu.roll(first, 1, 1), a[2]),
            last,
        ]

    for load in loads[:3]:
        load.wait()
    third = times(vin[256:], zt[...])
    for r in range(2):
        lines = times(vin[r * N : (r + 1) * N], zf[...]) + part(third, r)
        for n in range(8):
            s0[:, r * 8 + n, :] = lines[n * 16 : (n + 1) * 16]
    for p in range(2):
        ir4[p, pl.ds(KEPT * 4, (PAD - KEPT) * 4), :] = jnp.zeros(((PAD - KEPT) * 4, N), F32)
    ir3[pl.ds(KEPT * 3, (PAD - KEPT) * 3), :] = jnp.zeros(((PAD - KEPT) * 3, N), F32)

    pl.semaphore_wait(barrier, 22)
    for j in range(1, 8):
        pl.semaphore_signal(ready_sem, inc=1, device_id=(row, (col + j) % 8))
    row_exchange(s0, r0, 0)
    loads[3].wait()
    rows = [r0[:, r * 8 : (r + 1) * 8, :].reshape(N, N) for r in range(2)]
    low = jnp.where(
        lane == 0,
        pltpu.roll(rows[0], HALF, 1),
        jnp.where(
            lane % HALF < 22, pltpu.roll(rows[0], N - 42, 1), pltpu.roll(rows[1], N - 21, 1)
        ),
    )
    put_forward(
        0,
        x_forward(
            [
                jnp.where(lane == HALF, 0.0, rows[0]),
                rows[1],
                jnp.where(lane == HALF, 0.0, low),
            ]
        ),
    )
    pl.semaphore_wait(ready_sem, 7)
    send_forward(0)
    for load in loads[4:]:
        load.wait()

    @pl.when(active)
    def _():
        a = spectral(0)
        for c in range(3):
            a0[c] = a[c]
        scatter(with_curl(a), is4.at[0], 4)
        send_inverse(is4.at[0], ir4.at[0], 0, 4)

    for p in range(2):
        got = take_inverse(is4.at[p], ir4.at[p], p, 4)
        got.append(kz * got[0] - ky * got[2])
        lines = fold(x_inverse_pair(got), N, -1.0)
        u, w = [], [None, times(lines[4], zw[0]), times(lines[3], zw[1])]
        for c in range(3):
            pair = times(lines[c], zu[c])
            u.append(part(pair, 0))
            w[0] = part(pair, 1) if c == 0 else w[0] + part(pair, 1)
        product = [
            u[1] * w[2] - u[2] * w[1],
            u[2] * w[0] - u[0] * w[2],
            u[0] * w[1] - u[1] * w[0],
        ]
        put_forward(p + 1, x_forward([times(n, zf[...]) for n in product]))
        send_forward(p + 1)

        @pl.when(active)
        def _():
            b = spectral(p + 1)
            damp = norm() * (1.0 / N)
            if p == 0:
                nxt = []
                for c in range(3):
                    base = a0[c]
                    rate = b[c] - damp * base
                    acc[c] = base + (0.5 * STEP) * rate
                    nxt.append(base + STEP * rate)
                    a0[c] = nxt[c]
                scatter(with_curl(nxt), is4.at[1], 4)
                send_inverse(is4.at[1], ir4.at[1], 1, 4)
            else:
                last = []
                for c in range(3):
                    last.append(acc[c] + (0.5 * STEP) * (b[c] - damp * a0[c]))
                scatter(last, is3, 3)
                send_inverse(is3, ir3, 2, 3)

    got = take_inverse(is3, ir3, 2, 3)
    ends = fold(x_inverse_pair(got), N, -1.0)
    packed = [
        jnp.where(
            lane == HALF,
            pltpu.roll(ends[2], HALF, 1),
            jnp.where(spare, pltpu.roll(ends[2], 42, 1), ends[0]),
        ),
        jnp.where(spare, pltpu.roll(ends[2], 21, 1), ends[1]),
    ]
    for r in range(2):
        t0[:, r * 8 : (r + 1) * 8, :] = packed[r].reshape(16, 8, N)
    row_exchange(t0, q0, 1)
    pairs = [times(q0[:, r * 8 : (r + 1) * 8, :].reshape(N, N), zo[r]) for r in range(2)]
    final = [part(pairs[0], 0), part(pairs[1], 0), part(pairs[0], 1) + part(pairs[1], 1)]
    for y in range(16):
        for c in range(3):
            out[pl.ds(c * 128 + y, 8, stride=16), :] = final[c][y * 8 : y * 8 + 8]
    store = pltpu.make_async_copy(out, o_hbm, store_sem)
    store.start()

    for slot in range(2):
        pltpu.make_async_copy(s0.at[pl.ds(0, 15)], s0.at[pl.ds(0, 15)], row_s.at[slot]).wait()
    for p in range(3):
        @pl.when(active)
        def _():
            wait_rows(fs.at[p], (KEPT - 1) * 3, fwd_s.at[p])
            if p < 2:
                wait_rows(is4.at[p], 127 * 4, inv_s.at[p])
            else:
                wait_rows(is3, 127 * 3, inv_s.at[p])

        @pl.when(idle)
        def _():
            wait_rows(fs.at[p], KEPT * 3, fwd_s.at[p])

    store.wait()


def local(velocity):
    consts = tables()
    shapes = [((384, N), F32)] + [(t.shape, BF16) for t in consts]
    scratch = [VMEM(shape, kind) for shape, kind in shapes]
    scratch += [
        VMEM((16, 16, N), F32), VMEM((16, 16, N), F32),
        VMEM((3, PAD * 3, N), F32), VMEM((3, N * 3, N), F32),
        VMEM((2, N * 4, N), F32), VMEM((2, PAD * 4, N), F32),
        VMEM((N * 3, N), F32), VMEM((PAD * 3, N), F32),
        VMEM((16, 16, N), F32), VMEM((16, 16, N), F32),
        VMEM((384, N), F32), VMEM((3, PAD, N), F32), VMEM((3, PAD, N), F32),
        pltpu.SemaphoreType.DMA((8,)), pltpu.SemaphoreType.DMA(()),
        pltpu.SemaphoreType.REGULAR,
        pltpu.SemaphoreType.DMA((2,)), pltpu.SemaphoreType.DMA((2,)),
        pltpu.SemaphoreType.DMA((3,)), pltpu.SemaphoreType.DMA((3,)),
        pltpu.SemaphoreType.DMA((3,)), pltpu.SemaphoreType.DMA((3,)),
    ]
    anywhere = pl.BlockSpec(memory_space=pl.ANY)
    result = pl.pallas_call(
        kernel,
        out_shape=jax.ShapeDtypeStruct((384, N), F32),
        in_specs=[anywhere] * 8,
        out_specs=anywhere,
        scratch_shapes=scratch,
        compiler_params=pltpu.CompilerParams(collective_id=0, has_side_effects=True),
        name="heun",
    )(velocity.reshape(384, N), *[jnp.asarray(t) for t in consts])
    return result.reshape(3, 8, 16, N)


def solution(mesh):
    placed = (P(None, "row", "col", None),)
    return jax.shard_map(
        local, mesh=mesh, in_specs=placed, out_specs=P(None, "row", "col", None), check_vma=False
    )
```

```python
import itertools

import jax
import jax.numpy as jnp
import numpy as np
from jax import lax
from jax.experimental import pallas as pl
from jax.experimental.pallas import tpu as pltpu
from jax.sharding import PartitionSpec as P

N = 128
BAND = 43
KEPT = 85
PAD = 96
HALF = 64
F32 = jnp.float32
SPARE_AT = 0
BF16 = jnp.bfloat16
VMEM = pltpu.VMEM
STEP = 2.0 / N
MOVES = sorted(
    itertools.product(range(4), repeat=3), key=lambda move: -sum((0, 1, 2, 1)[d] for d in move)
)
ROW_MOVES = [move for move in itertools.product(range(4), range(2), range(2)) if any(move)]
ROW_MOVES.sort(key=lambda move: -((0, 1, 2, 1)[move[0]] + 2 * move[1]))


def split_np(table):
    high = table.astype(np.float32).astype(BF16)
    low = (table - high.astype(np.float64)).astype(np.float32).astype(BF16)
    return high, low


def tables():
    turn = 2.0 * np.pi / N
    cell = np.arange(N)
    kz = np.arange(BAND)
    angle_z = turn * ((cell[:, None] * kz[None, :]) % N)
    z_forward = np.zeros((N, N))
    z_forward[:, :BAND] = np.cos(angle_z) / N
    z_forward[:, HALF : HALF + BAND] = -np.sin(angle_z) / N
    weight = np.where(kz == 0, 1.0, 2.0)
    z_inverse = np.zeros((N, N))
    z_inverse[:BAND] = (np.cos(angle_z) * weight).T
    z_inverse[HALF : HALF + BAND] = (-np.sin(angle_z) * weight).T
    z_turned = np.concatenate([z_inverse[HALF:], -z_inverse[:HALF]])

    def spares(first, count):
        lanes = np.arange(count) + BAND
        waves = np.arange(count) + first
        return np.concatenate([lanes, lanes + HALF]), np.concatenate([waves, waves + HALF])

    z_third = np.zeros((2, N, N))
    z_third_back = np.zeros((2, N, N))
    for r in range(2):
        lanes, waves = spares(1 + 21 * r, 21)
        z_third[r][:, lanes] = z_forward[:, waves]
        z_third_back[r][lanes] = z_inverse[waves]
    z_third[0][:, HALF] = z_forward[:, 0]
    z_third_back[0][HALF] = z_inverse[0]
    z_fifth = np.zeros((3, N, N))
    for r, count in enumerate((21, 21, 1)):
        lanes, waves = spares(21 * r, count)
        z_fifth[r][lanes] = z_inverse[waves]
    wave = np.arange(KEPT)
    wave = np.where(wave < BAND, wave, wave - KEPT)
    angle = turn * ((wave[:, None] * cell[None, :]) % N)
    forward = np.zeros((2 * PAD, N))
    forward[:KEPT] = np.cos(angle) / N
    forward[PAD : PAD + KEPT] = np.sin(angle) / N
    inverse = np.zeros((2 * N, PAD))
    inverse[:N, :KEPT] = np.cos(angle).T
    inverse[N:, :KEPT] = np.sin(angle).T

    def left(table):
        high, low = split_np(table)
        return np.concatenate([high, high, low], axis=1)

    def right(table):
        high, low = split_np(table)
        return np.concatenate([high, high, low], axis=0)

    def beside(one, other):
        return right(np.concatenate([one, other], axis=1))

    return (
        right(z_forward),
        beside(z_third[0], z_third[1]),
        left(forward),
        left(inverse),
        np.stack([beside(z_inverse, z_fifth[r]) for r in range(3)]),
        np.stack([right(z_turned), right(z_inverse)]),
        np.stack([beside(z_inverse, z_third_back[r]) for r in range(2)]),
    )


def halves(value):
    high = value.astype(BF16)
    low = (value - high.astype(F32)).astype(BF16)
    return high, low


def times(value, table):
    high, low = halves(value)
    return jnp.dot(
        jnp.concatenate([high, low, high], axis=1), table, preferred_element_type=F32
    )


def under(table, value):
    high, low = halves(value)
    return jnp.dot(
        table, jnp.concatenate([high, low, high], axis=0), preferred_element_type=F32
    )


def column_of(row, col):
    chip = (row // 2) * 8 + col
    spare = jnp.where((chip % 3 == 0) & (chip < 63), 64 + chip // 3, 4096)
    return jnp.where(row % 2 == 1, chip, spare)


def kernel(
    v_hbm, zf_hbm, zt_hbm, xf_hbm, xi_hbm, zu_hbm, zw_hbm, zo_hbm, o_hbm,
    vin, zf, zt, xf, xi, zu, zw, zo, s0, r0, fs, fr, is4, ir4, is3, ir3, t0, q0, out, a0, acc,
    load_sem, store_sem, ready_sem, row_s, row_r, fwd_s, fwd_r, inv_s, inv_r,
):
    row, col = lax.axis_index("row"), lax.axis_index("col")
    me = col * 16 + row
    ki = column_of(row, col)
    active = ki < KEPT
    idle = jnp.logical_not(active)

    loads = [
        pltpu.make_async_copy(src, dst, load_sem.at[n])
        for n, (src, dst) in enumerate(
            [
                (v_hbm, vin), (zf_hbm, zf), (zt_hbm, zt), (xf_hbm, xf), (xi_hbm, xi),
                (zu_hbm, zu), (zw_hbm, zw), (zo_hbm, zo),
            ]
        )
    ]
    for load in loads:
        load.start()

    barrier = pltpu.get_barrier_semaphore()
    for j in range(1, 16):
        pl.semaphore_signal(barrier, inc=1, device_id=((row + j) % 16, col))
    for j in range(1, 8):
        pl.semaphore_signal(barrier, inc=1, device_id=(row, (col + j) % 8))

    z_at, y_at, x_at, core = row // 4, (row // 2 % 2) * 2 + col // 4, col % 4, row % 2
    lane = lax.broadcasted_iota(jnp.int32, (1, N), 1)
    side = jnp.where(lane < HALF, 1.0, -1.0).astype(F32)

    def turned(value):
        return pltpu.roll(value, HALF, 1) * side

    def part(value, c):
        return value[:, c * N : (c + 1) * N]

    def fold(both, rows, sign):
        outs = []
        for c in range(both.shape[1] // N):
            piece = part(both, c)
            outs.append(piece[:rows] + sign * turned(piece[rows:]))
        return outs

    def x_forward(parts):
        return fold(under(xf[...], jnp.concatenate(parts, axis=1)), PAD, 1.0)

    def x_inverse_pair(parts):
        return under(xi[...], jnp.concatenate(parts, axis=1))

    def row_exchange(src, dst, slot):
        for move in ROW_MOVES:
            to = (
                (z_at + move[0]) % 4 * 4
                + (row // 2 + move[1]) % 2 * 2
                + (core + move[2]) % 2
            )
            pltpu.make_async_remote_copy(
                src.at[to], dst.at[row], row_s.at[slot], row_r.at[slot], device_id=(to, col)
            ).start()
        dst[row] = src[row]
        pltpu.make_async_copy(
            dst.at[pl.ds(0, 15)], dst.at[pl.ds(0, 15)], row_r.at[slot]
        ).wait()

    def copy_rows(src, at, dst, to, rows):
        for n in range(rows):
            dst[pl.ds(to * rows + n, 1), :] = src[pl.ds(at * rows + n, 1), :]

    def wait_rows(ref, count, sem):
        pltpu.make_async_copy(ref.at[pl.ds(0, count)], ref.at[pl.ds(0, count)], sem).wait()

    def chip_at(move):
        z, y, x = (z_at + move[0]) % 4, (y_at + move[1]) % 4, (x_at + move[2]) % 4
        return z * 4 + (y // 2) * 2, (y % 2) * 4 + x

    def send_forward(p):
        def one(i, to):
            pltpu.make_async_remote_copy(
                fs.at[p, pl.ds(i * 3, 3)], fr.at[p, pl.ds(me * 3, 3)],
                fwd_s.at[p], fwd_r.at[p], device_id=to,
            ).start()

        own = (row // 2) * 8 + col
        first = (own // 3) % (KEPT - 64)

        def to_spare(turn):
            n = (first + turn) % (KEPT - 64)
            chip = n * 3
            one(64 + n, ((chip // 8) * 2, chip % 8))

        for at, move in enumerate(MOVES):
            if at == SPARE_AT:
                @pl.when(ki != 64 + first)
                def _():
                    to_spare(0)

                for turn in range(1, KEPT - 64):
                    to_spare(turn)
            base, side_col = chip_at(move)
            chip = (base // 2) * 8 + side_col
            if move == (0, 0, 0):
                @pl.when(core == 0)
                def _():
                    one(chip, (base + 1, side_col))
            else:
                one(chip, (base + 1, side_col))

    def put_forward(p, parts):
        for c in range(3):
            fs[p, pl.ds(c, PAD, stride=3), :] = parts[c]

    def take_forward(p):
        copy_rows(fs.at[p], ki, fr.at[p], me, 3)
        wait_rows(fr.at[p], 127 * 3, fwd_r.at[p])
        return [fr[p, pl.ds(c, N, stride=3), :] for c in range(3)]

    def send_inverse(src, dst, p, rows):
        def one(to):
            d = to[1] * 16 + to[0]
            pltpu.make_async_remote_copy(
                src.at[pl.ds(d * rows, rows)], dst.at[pl.ds(ki * rows, rows)],
                inv_s.at[p], inv_r.at[p], device_id=to,
            ).start()

        for move in MOVES:
            base, side_col = chip_at(move)
            for other in range(2):
                if move != (0, 0, 0) or other:
                    one((base + (core + other) % 2, side_col))

    def take_inverse(src, dst, p, rows):
        @pl.when(active)
        def _():
            copy_rows(src, me, dst, ki, rows)
            wait_rows(dst, (KEPT - 1) * rows, inv_r.at[p])

        @pl.when(idle)
        def _():
            wait_rows(dst, KEPT * rows, inv_r.at[p])

        return [dst[pl.ds(c, PAD, stride=rows), :] for c in range(rows)]

    kx = jnp.where(ki < BAND, ki, ki - KEPT).astype(F32)
    ky_at = lax.broadcasted_iota(jnp.int32, (PAD, N), 0)
    ky = jnp.where(ky_at < BAND, ky_at, ky_at - KEPT).astype(F32)
    kz = (lax.broadcasted_iota(jnp.int32, (PAD, N), 1) % HALF).astype(F32)

    def norm():
        return kx * kx + ky * ky + kz * kz

    def spectral(p):
        b = x_forward(take_forward(p))
        squared = norm()
        along = (kx * b[0] + ky * b[1] + kz * b[2]) / jnp.where(squared > 0, squared, 1.0)
        return [b[0] - kx * along, b[1] - ky * along, b[2] - kz * along]

    def scatter(state, ref, rows):
        outs = fold(x_inverse_pair(state), N, -1.0)
        for c in range(rows):
            ref[pl.ds(c, N, stride=rows), :] = outs[c]

    spare = lane % HALF >= BAND

    def with_curl(a):
        first = -turned(ky * a[2] - kz * a[1])
        last = -turned(kx * a[1] - ky * a[0])
        return [
            jnp.where(spare, pltpu.roll(first, BAND, 1), a[0]),
            jnp.where(spare, pltpu.roll(first, BAND - 21, 1), a[1]),
            jnp.where(spare, pltpu.roll(first, 1, 1), a[2]),
            last,
        ]

    for load in loads[:3]:
        load.wait()
    third = times(vin[256:], zt[...])
    for r in range(2):
        lines = times(vin[r * N : (r + 1) * N], zf[...]) + part(third, r)
        for n in range(8):
            s0[:, r * 8 + n, :] = lines[n * 16 : (n + 1) * 16]
    for p in range(2):
        ir4[p, pl.ds(KEPT * 4, (PAD - KEPT) * 4), :] = jnp.zeros(((PAD - KEPT) * 4, N), F32)
    ir3[pl.ds(KEPT * 3, (PAD - KEPT) * 3), :] = jnp.zeros(((PAD - KEPT) * 3, N), F32)

    pl.semaphore_wait(barrier, 22)
    for j in range(1, 8):
        pl.semaphore_signal(ready_sem, inc=1, device_id=(row, (col + j) % 8))
    row_exchange(s0, r0, 0)
    loads[3].wait()
    rows = [r0[:, r * 8 : (r + 1) * 8, :].reshape(N, N) for r in range(2)]
    low = jnp.where(
        lane == 0,
        pltpu.roll(rows[0], HALF, 1),
        jnp.where(
            lane % HALF < 22, pltpu.roll(rows[0], N - 42, 1), pltpu.roll(rows[1], N - 21, 1)
        ),
    )
    put_forward(
        0,
        x_forward(
            [
                jnp.where(lane == HALF, 0.0, rows[0]),
                rows[1],
                jnp.where(lane == HALF, 0.0, low),
            ]
        ),
    )
    pl.semaphore_wait(ready_sem, 7)
    send_forward(0)
    for load in loads[4:]:
        load.wait()

    @pl.when(active)
    def _():
        a = spectral(0)
        for c in range(3):
            a0[c] = a[c]
        scatter(with_curl(a), is4.at[0], 4)
        send_inverse(is4.at[0], ir4.at[0], 0, 4)

    for p in range(2):
        got = take_inverse(is4.at[p], ir4.at[p], p, 4)
        got.append(kz * got[0] - ky * got[2])
        lines = fold(x_inverse_pair(got), N, -1.0)
        u, w = [], [None, times(lines[4], zw[0]), times(lines[3], zw[1])]
        for c in range(3):
            pair = times(lines[c], zu[c])
            u.append(part(pair, 0))
            w[0] = part(pair, 1) if c == 0 else w[0] + part(pair, 1)
        product = [
            u[1] * w[2] - u[2] * w[1],
            u[2] * w[0] - u[0] * w[2],
            u[0] * w[1] - u[1] * w[0],
        ]
        put_forward(p + 1, x_forward([times(n, zf[...]) for n in product]))
        send_forward(p + 1)

        @pl.when(active)
        def _():
            b = spectral(p + 1)
            damp = norm() * (1.0 / N)
            if p == 0:
                nxt = []
                for c in range(3):
                    base = a0[c]
                    rate = b[c] - damp * base
                    acc[c] = base + (0.5 * STEP) * rate
                    nxt.append(base + STEP * rate)
                    a0[c] = nxt[c]
                scatter(with_curl(nxt), is4.at[1], 4)
                send_inverse(is4.at[1], ir4.at[1], 1, 4)
            else:
                last = []
                for c in range(3):
                    last.append(acc[c] + (0.5 * STEP) * (b[c] - damp * a0[c]))
                scatter(last, is3, 3)
                send_inverse(is3, ir3, 2, 3)

    got = take_inverse(is3, ir3, 2, 3)
    ends = fold(x_inverse_pair(got), N, -1.0)
    packed = [
        jnp.where(
            lane == HALF,
            pltpu.roll(ends[2], HALF, 1),
            jnp.where(spare, pltpu.roll(ends[2], 42, 1), ends[0]),
        ),
        jnp.where(spare, pltpu.roll(ends[2], 21, 1), ends[1]),
    ]
    for r in range(2):
        t0[:, r * 8 : (r + 1) * 8, :] = packed[r].reshape(16, 8, N)
    row_exchange(t0, q0, 1)
    pairs = [times(q0[:, r * 8 : (r + 1) * 8, :].reshape(N, N), zo[r]) for r in range(2)]
    final = [part(pairs[0], 0), part(pairs[1], 0), part(pairs[0], 1) + part(pairs[1], 1)]
    for y in range(16):
        for c in range(3):
            out[pl.ds(c * 128 + y, 8, stride=16), :] = final[c][y * 8 : y * 8 + 8]
    store = pltpu.make_async_copy(out, o_hbm, store_sem)
    store.start()

    for slot in range(2):
        pltpu.make_async_copy(s0.at[pl.ds(0, 15)], s0.at[pl.ds(0, 15)], row_s.at[slot]).wait()
    for p in range(3):
        @pl.when(active)
        def _():
            wait_rows(fs.at[p], (KEPT - 1) * 3, fwd_s.at[p])
            if p < 2:
                wait_rows(is4.at[p], 127 * 4, inv_s.at[p])
            else:
                wait_rows(is3, 127 * 3, inv_s.at[p])

        @pl.when(idle)
        def _():
            wait_rows(fs.at[p], KEPT * 3, fwd_s.at[p])

    store.wait()


def local(velocity):
    consts = tables()
    shapes = [((384, N), F32)] + [(t.shape, BF16) for t in consts]
    scratch = [VMEM(shape, kind) for shape, kind in shapes]
    scratch += [
        VMEM((16, 16, N), F32), VMEM((16, 16, N), F32),
        VMEM((3, PAD * 3, N), F32), VMEM((3, N * 3, N), F32),
        VMEM((2, N * 4, N), F32), VMEM((2, PAD * 4, N), F32),
        VMEM((N * 3, N), F32), VMEM((PAD * 3, N), F32),
        VMEM((16, 16, N), F32), VMEM((16, 16, N), F32),
        VMEM((384, N), F32), VMEM((3, PAD, N), F32), VMEM((3, PAD, N), F32),
        pltpu.SemaphoreType.DMA((8,)), pltpu.SemaphoreType.DMA(()),
        pltpu.SemaphoreType.REGULAR,
        pltpu.SemaphoreType.DMA((2,)), pltpu.SemaphoreType.DMA((2,)),
        pltpu.SemaphoreType.DMA((3,)), pltpu.SemaphoreType.DMA((3,)),
        pltpu.SemaphoreType.DMA((3,)), pltpu.SemaphoreType.DMA((3,)),
    ]
    anywhere = pl.BlockSpec(memory_space=pl.ANY)
    result = pl.pallas_call(
        kernel,
        out_shape=jax.ShapeDtypeStruct((384, N), F32),
        in_specs=[anywhere] * 8,
        out_specs=anywhere,
        scratch_shapes=scratch,
        compiler_params=pltpu.CompilerParams(collective_id=0, has_side_effects=True),
        name="heun",
    )(velocity.reshape(384, N), *[jnp.asarray(t) for t in consts])
    return result.reshape(3, 8, 16, N)


def solution(mesh):
    placed = (P(None, "row", "col", None),)
    return jax.shard_map(
        local, mesh=mesh, in_specs=placed, out_specs=P(None, "row", "col", None), check_vma=False
    )
```

```python
import itertools

import jax
import jax.numpy as jnp
import numpy as np
from jax import lax
from jax.experimental import pallas as pl
from jax.experimental.pallas import tpu as pltpu
from jax.sharding import PartitionSpec as P

N = 128
BAND = 43
KEPT = 85
PAD = 96
HALF = 64
F32 = jnp.float32
SPARE_AT = 0
BF16 = jnp.bfloat16
VMEM = pltpu.VMEM
STEP = 2.0 / N
MOVES = sorted(
    itertools.product(range(4), repeat=3), key=lambda move: -sum((0, 1, 2, 1)[d] for d in move)
)
TARGETS = sorted(
    itertools.product(MOVES[:-1], range(2)),
    key=lambda to: -sum((0, 1, 2, 1)[d] for d in to[0]) - 0.6 * (1 - to[1]),
)
ROW_MOVES = [move for move in itertools.product(range(4), range(2), range(2)) if any(move)]
ROW_MOVES.sort(key=lambda move: -((0, 1, 2, 1)[move[0]] + 2 * move[1]))


def split_np(table):
    high = table.astype(np.float32).astype(BF16)
    low = (table - high.astype(np.float64)).astype(np.float32).astype(BF16)
    return high, low


def tables():
    turn = 2.0 * np.pi / N
    cell = np.arange(N)
    kz = np.arange(BAND)
    angle_z = turn * ((cell[:, None] * kz[None, :]) % N)
    z_forward = np.zeros((N, N))
    z_forward[:, :BAND] = np.cos(angle_z) / N
    z_forward[:, HALF : HALF + BAND] = -np.sin(angle_z) / N
    weight = np.where(kz == 0, 1.0, 2.0)
    z_inverse = np.zeros((N, N))
    z_inverse[:BAND] = (np.cos(angle_z) * weight).T
    z_inverse[HALF : HALF + BAND] = (-np.sin(angle_z) * weight).T
    z_turned = np.concatenate([z_inverse[HALF:], -z_inverse[:HALF]])

    def spares(first, count):
        lanes = np.arange(count) + BAND
        waves = np.arange(count) + first
        return np.concatenate([lanes, lanes + HALF]), np.concatenate([waves, waves + HALF])

    z_third = np.zeros((2, N, N))
    z_third_back = np.zeros((2, N, N))
    for r in range(2):
        lanes, waves = spares(1 + 21 * r, 21)
        z_third[r][:, lanes] = z_forward[:, waves]
        z_third_back[r][lanes] = z_inverse[waves]
    z_third[0][:, HALF] = z_forward[:, 0]
    z_third_back[0][HALF] = z_inverse[0]
    z_fifth = np.zeros((3, N, N))
    for r, count in enumerate((21, 21, 1)):
        lanes, waves = spares(21 * r, count)
        z_fifth[r][lanes] = z_inverse[waves]
    wave = np.arange(KEPT)
    wave = np.where(wave < BAND, wave, wave - KEPT)
    angle = turn * ((wave[:, None] * cell[None, :]) % N)
    forward = np.zeros((2 * PAD, N))
    forward[:KEPT] = np.cos(angle) / N
    forward[PAD : PAD + KEPT] = np.sin(angle) / N
    inverse = np.zeros((2 * N, PAD))
    inverse[:N, :KEPT] = np.cos(angle).T
    inverse[N:, :KEPT] = np.sin(angle).T

    def left(table):
        high, low = split_np(table)
        return np.concatenate([high, high, low], axis=1)

    def right(table):
        high, low = split_np(table)
        return np.concatenate([high, high, low], axis=0)

    def beside(one, other):
        return right(np.concatenate([one, other], axis=1))

    return (
        right(z_forward),
        beside(z_third[0], z_third[1]),
        left(forward),
        left(inverse),
        np.stack([beside(z_inverse, z_fifth[r]) for r in range(3)]),
        np.stack([right(z_turned), right(z_inverse)]),
        np.stack([beside(z_inverse, z_third_back[r]) for r in range(2)]),
    )


def halves(value):
    high = value.astype(BF16)
    low = (value - high.astype(F32)).astype(BF16)
    return high, low


def times(value, table):
    high, low = halves(value)
    return jnp.dot(
        jnp.concatenate([high, low, high], axis=1), table, preferred_element_type=F32
    )


def under(table, value):
    high, low = halves(value)
    return jnp.dot(
        table, jnp.concatenate([high, low, high], axis=0), preferred_element_type=F32
    )


def column_of(row, col):
    chip = (row // 2) * 8 + col
    spare = jnp.where((chip % 3 == 0) & (chip < 63), 64 + chip // 3, 4096)
    return jnp.where(row % 2 == 1, chip, spare)


def kernel(
    v_hbm, zf_hbm, zt_hbm, xf_hbm, xi_hbm, zu_hbm, zw_hbm, zo_hbm, o_hbm,
    vin, zf, zt, xf, xi, zu, zw, zo, s0, r0, fs, fr, is4, ir4, is3, ir3, t0, q0, out, a0, acc,
    load_sem, store_sem, ready_sem, row_s, row_r, fwd_s, fwd_r, inv_s, inv_r,
):
    row, col = lax.axis_index("row"), lax.axis_index("col")
    me = col * 16 + row
    ki = column_of(row, col)
    active = ki < KEPT
    idle = jnp.logical_not(active)

    loads = [
        pltpu.make_async_copy(src, dst, load_sem.at[n])
        for n, (src, dst) in enumerate(
            [
                (v_hbm, vin), (zf_hbm, zf), (zt_hbm, zt), (xf_hbm, xf), (xi_hbm, xi),
                (zu_hbm, zu), (zw_hbm, zw), (zo_hbm, zo),
            ]
        )
    ]
    for load in loads:
        load.start()

    barrier = pltpu.get_barrier_semaphore()
    for j in range(1, 16):
        pl.semaphore_signal(barrier, inc=1, device_id=((row + j) % 16, col))
    for j in range(1, 8):
        pl.semaphore_signal(barrier, inc=1, device_id=(row, (col + j) % 8))

    z_at, y_at, x_at, core = row // 4, (row // 2 % 2) * 2 + col // 4, col % 4, row % 2
    lane = lax.broadcasted_iota(jnp.int32, (1, N), 1)
    side = jnp.where(lane < HALF, 1.0, -1.0).astype(F32)

    def turned(value):
        return pltpu.roll(value, HALF, 1) * side

    def part(value, c):
        return value[:, c * N : (c + 1) * N]

    def fold(both, rows, sign):
        outs = []
        for c in range(both.shape[1] // N):
            piece = part(both, c)
            outs.append(piece[:rows] + sign * turned(piece[rows:]))
        return outs

    def x_forward(parts):
        return fold(under(xf[...], jnp.concatenate(parts, axis=1)), PAD, 1.0)

    def x_inverse_pair(parts):
        return under(xi[...], jnp.concatenate(parts, axis=1))

    def row_exchange(src, dst, slot):
        for move in ROW_MOVES:
            to = (
                (z_at + move[0]) % 4 * 4
                + (row // 2 + move[1]) % 2 * 2
                + (core + move[2]) % 2
            )
            pltpu.make_async_remote_copy(
                src.at[to], dst.at[row], row_s.at[slot], row_r.at[slot], device_id=(to, col)
            ).start()
        dst[row] = src[row]
        pltpu.make_async_copy(
            dst.at[pl.ds(0, 15)], dst.at[pl.ds(0, 15)], row_r.at[slot]
        ).wait()

    def copy_rows(src, at, dst, to, rows):
        for n in range(rows):
            dst[pl.ds(to * rows + n, 1), :] = src[pl.ds(at * rows + n, 1), :]

    def wait_rows(ref, count, sem):
        pltpu.make_async_copy(ref.at[pl.ds(0, count)], ref.at[pl.ds(0, count)], sem).wait()

    def chip_at(move):
        z, y, x = (z_at + move[0]) % 4, (y_at + move[1]) % 4, (x_at + move[2]) % 4
        return z * 4 + (y // 2) * 2, (y % 2) * 4 + x

    def send_forward(p):
        def one(i, to):
            pltpu.make_async_remote_copy(
                fs.at[p, pl.ds(i * 3, 3)], fr.at[p, pl.ds(me * 3, 3)],
                fwd_s.at[p], fwd_r.at[p], device_id=to,
            ).start()

        own = (row // 2) * 8 + col
        first = (own // 3) % (KEPT - 64)

        def to_spare(turn):
            n = (first + turn) % (KEPT - 64)
            chip = n * 3
            one(64 + n, ((chip // 8) * 2, chip % 8))

        for at, move in enumerate(MOVES):
            if at == SPARE_AT:
                @pl.when(ki != 64 + first)
                def _():
                    to_spare(0)

                for turn in range(1, KEPT - 64):
                    to_spare(turn)
            base, side_col = chip_at(move)
            chip = (base // 2) * 8 + side_col
            if move == (0, 0, 0):
                @pl.when(core == 0)
                def _():
                    one(chip, (base + 1, side_col))
            else:
                one(chip, (base + 1, side_col))

    def put_forward(p, parts):
        for c in range(3):
            fs[p, pl.ds(c, PAD, stride=3), :] = parts[c]

    def take_forward(p):
        copy_rows(fs.at[p], ki, fr.at[p], me, 3)
        wait_rows(fr.at[p], 127 * 3, fwd_r.at[p])
        return [fr[p, pl.ds(c, N, stride=3), :] for c in range(3)]

    def send_inverse(src, dst, p, rows):
        def one(to):
            d = to[1] * 16 + to[0]
            pltpu.make_async_remote_copy(
                src.at[pl.ds(d * rows, rows)], dst.at[pl.ds(ki * rows, rows)],
                inv_s.at[p], inv_r.at[p], device_id=to,
            ).start()

        for move, to_core in TARGETS:
            base, side_col = chip_at(move)
            one((base + to_core, side_col))
        one((row + 1 - 2 * core, col))

    def take_inverse(src, dst, p, rows):
        @pl.when(active)
        def _():
            copy_rows(src, me, dst, ki, rows)
            wait_rows(dst, (KEPT - 1) * rows, inv_r.at[p])

        @pl.when(idle)
        def _():
            wait_rows(dst, KEPT * rows, inv_r.at[p])

        return [dst[pl.ds(c, PAD, stride=rows), :] for c in range(rows)]

    kx = jnp.where(ki < BAND, ki, ki - KEPT).astype(F32)
    ky_at = lax.broadcasted_iota(jnp.int32, (PAD, N), 0)
    ky = jnp.where(ky_at < BAND, ky_at, ky_at - KEPT).astype(F32)
    kz = (lax.broadcasted_iota(jnp.int32, (PAD, N), 1) % HALF).astype(F32)

    def norm():
        return kx * kx + ky * ky + kz * kz

    def spectral(p):
        b = x_forward(take_forward(p))
        squared = norm()
        along = (kx * b[0] + ky * b[1] + kz * b[2]) / jnp.where(squared > 0, squared, 1.0)
        return [b[0] - kx * along, b[1] - ky * along, b[2] - kz * along]

    def scatter(state, ref, rows):
        outs = fold(x_inverse_pair(state), N, -1.0)
        for c in range(rows):
            ref[pl.ds(c, N, stride=rows), :] = outs[c]

    spare = lane % HALF >= BAND

    def with_curl(a):
        first = -turned(ky * a[2] - kz * a[1])
        last = -turned(kx * a[1] - ky * a[0])
        return [
            jnp.where(spare, pltpu.roll(first, BAND, 1), a[0]),
            jnp.where(spare, pltpu.roll(first, BAND - 21, 1), a[1]),
            jnp.where(spare, pltpu.roll(first, 1, 1), a[2]),
            last,
        ]

    for load in loads[:3]:
        load.wait()
    third = times(vin[256:], zt[...])
    for r in range(2):
        lines = times(vin[r * N : (r + 1) * N], zf[...]) + part(third, r)
        for n in range(8):
            s0[:, r * 8 + n, :] = lines[n * 16 : (n + 1) * 16]
    for p in range(2):
        ir4[p, pl.ds(KEPT * 4, (PAD - KEPT) * 4), :] = jnp.zeros(((PAD - KEPT) * 4, N), F32)
    ir3[pl.ds(KEPT * 3, (PAD - KEPT) * 3), :] = jnp.zeros(((PAD - KEPT) * 3, N), F32)

    pl.semaphore_wait(barrier, 22)
    for j in range(1, 8):
        pl.semaphore_signal(ready_sem, inc=1, device_id=(row, (col + j) % 8))
    row_exchange(s0, r0, 0)
    loads[3].wait()
    rows = [r0[:, r * 8 : (r + 1) * 8, :].reshape(N, N) for r in range(2)]
    low = jnp.where(
        lane == 0,
        pltpu.roll(rows[0], HALF, 1),
        jnp.where(
            lane % HALF < 22, pltpu.roll(rows[0], N - 42, 1), pltpu.roll(rows[1], N - 21, 1)
        ),
    )
    put_forward(
        0,
        x_forward(
            [
                jnp.where(lane == HALF, 0.0, rows[0]),
                rows[1],
                jnp.where(lane == HALF, 0.0, low),
            ]
        ),
    )
    pl.semaphore_wait(ready_sem, 7)
    send_forward(0)
    for load in loads[4:]:
        load.wait()

    @pl.when(active)
    def _():
        a = spectral(0)
        for c in range(3):
            a0[c] = a[c]
        scatter(with_curl(a), is4.at[0], 4)
        send_inverse(is4.at[0], ir4.at[0], 0, 4)

    for p in range(2):
        got = take_inverse(is4.at[p], ir4.at[p], p, 4)
        got.append(kz * got[0] - ky * got[2])
        lines = fold(x_inverse_pair(got), N, -1.0)
        u, w = [], [None, times(lines[4], zw[0]), times(lines[3], zw[1])]
        for c in range(3):
            pair = times(lines[c], zu[c])
            u.append(part(pair, 0))
            w[0] = part(pair, 1) if c == 0 else w[0] + part(pair, 1)
        product = [
            u[1] * w[2] - u[2] * w[1],
            u[2] * w[0] - u[0] * w[2],
            u[0] * w[1] - u[1] * w[0],
        ]
        put_forward(p + 1, x_forward([times(n, zf[...]) for n in product]))
        send_forward(p + 1)

        @pl.when(active)
        def _():
            b = spectral(p + 1)
            damp = norm() * (1.0 / N)
            if p == 0:
                nxt = []
                for c in range(3):
                    base = a0[c]
                    rate = b[c] - damp * base
                    acc[c] = base + (0.5 * STEP) * rate
                    nxt.append(base + STEP * rate)
                    a0[c] = nxt[c]
                scatter(with_curl(nxt), is4.at[1], 4)
                send_inverse(is4.at[1], ir4.at[1], 1, 4)
            else:
                last = []
                for c in range(3):
                    last.append(acc[c] + (0.5 * STEP) * (b[c] - damp * a0[c]))
                scatter(last, is3, 3)
                send_inverse(is3, ir3, 2, 3)

    got = take_inverse(is3, ir3, 2, 3)
    ends = fold(x_inverse_pair(got), N, -1.0)
    packed = [
        jnp.where(
            lane == HALF,
            pltpu.roll(ends[2], HALF, 1),
            jnp.where(spare, pltpu.roll(ends[2], 42, 1), ends[0]),
        ),
        jnp.where(spare, pltpu.roll(ends[2], 21, 1), ends[1]),
    ]
    for r in range(2):
        t0[:, r * 8 : (r + 1) * 8, :] = packed[r].reshape(16, 8, N)
    row_exchange(t0, q0, 1)
    pairs = [times(q0[:, r * 8 : (r + 1) * 8, :].reshape(N, N), zo[r]) for r in range(2)]
    final = [part(pairs[0], 0), part(pairs[1], 0), part(pairs[0], 1) + part(pairs[1], 1)]
    for y in range(16):
        for c in range(3):
            out[pl.ds(c * 128 + y, 8, stride=16), :] = final[c][y * 8 : y * 8 + 8]
    store = pltpu.make_async_copy(out, o_hbm, store_sem)
    store.start()

    for slot in range(2):
        pltpu.make_async_copy(s0.at[pl.ds(0, 15)], s0.at[pl.ds(0, 15)], row_s.at[slot]).wait()
    for p in range(3):
        @pl.when(active)
        def _():
            wait_rows(fs.at[p], (KEPT - 1) * 3, fwd_s.at[p])
            if p < 2:
                wait_rows(is4.at[p], 127 * 4, inv_s.at[p])
            else:
                wait_rows(is3, 127 * 3, inv_s.at[p])

        @pl.when(idle)
        def _():
            wait_rows(fs.at[p], KEPT * 3, fwd_s.at[p])

    store.wait()


def local(velocity):
    consts = tables()
    shapes = [((384, N), F32)] + [(t.shape, BF16) for t in consts]
    scratch = [VMEM(shape, kind) for shape, kind in shapes]
    scratch += [
        VMEM((16, 16, N), F32), VMEM((16, 16, N), F32),
        VMEM((3, PAD * 3, N), F32), VMEM((3, N * 3, N), F32),
        VMEM((2, N * 4, N), F32), VMEM((2, PAD * 4, N), F32),
        VMEM((N * 3, N), F32), VMEM((PAD * 3, N), F32),
        VMEM((16, 16, N), F32), VMEM((16, 16, N), F32),
        VMEM((384, N), F32), VMEM((3, PAD, N), F32), VMEM((3, PAD, N), F32),
        pltpu.SemaphoreType.DMA((8,)), pltpu.SemaphoreType.DMA(()),
        pltpu.SemaphoreType.REGULAR,
        pltpu.SemaphoreType.DMA((2,)), pltpu.SemaphoreType.DMA((2,)),
        pltpu.SemaphoreType.DMA((3,)), pltpu.SemaphoreType.DMA((3,)),
        pltpu.SemaphoreType.DMA((3,)), pltpu.SemaphoreType.DMA((3,)),
    ]
    anywhere = pl.BlockSpec(memory_space=pl.ANY)
    result = pl.pallas_call(
        kernel,
        out_shape=jax.ShapeDtypeStruct((384, N), F32),
        in_specs=[anywhere] * 8,
        out_specs=anywhere,
        scratch_shapes=scratch,
        compiler_params=pltpu.CompilerParams(collective_id=0, has_side_effects=True),
        name="heun",
    )(velocity.reshape(384, N), *[jnp.asarray(t) for t in consts])
    return result.reshape(3, 8, 16, N)


def solution(mesh):
    placed = (P(None, "row", "col", None),)
    return jax.shard_map(
        local, mesh=mesh, in_specs=placed, out_specs=P(None, "row", "col", None), check_vma=False
    )
```
